32 devices in a mesh: heads: 4 (over y, core), blk: 8 (over z, x).
Axes of the slice: x: 2, y: 2, z: 4, core: 2. Of those that a mesh axis runs over, the one named last changes fastest.
Arguments:
- tokens: bfloat16 [4096, 4096], P(('blk', 'heads')), may hold values from -6 to 6
- w_query: bfloat16 [4096, 2048], P('blk', 'heads'), may hold values from -0.75 to 0.75
- key_value_weight: bfloat16 [4096, 2, 512], P('blk', None, 'heads'), may hold values from -0.75 to 0.75
- w_out: bfloat16 [2048, 4096], P(('heads', 'blk')), may hold values from -0.5 to 0.5
- doc_lengths: int32 [16], replicated, may hold values from 1 to 1024, 4096 in all
Outputs:
- attended: bfloat16 [4096, 4096], P(('blk', 'heads'))
The draws below stay inside these ranges and needn't reach their ends.
Inputs may be any that keep to these rules, and one draw needn't show every extreme that they name: `doc_lengths`: the 16 lengths sum to 4096; the longest document has exactly 1024 tokens.
All inputs are finite; a program needn't handle non-finite values.
Results may differ from the reference program's by a relative error of at most 0.012.
Values may be sent and summed in bfloat16 or wider, within the bound.
A program may use at most 128 MiB of HBM per device.

```python
import math
import jax
import jax.numpy as jnp
import numpy as np
from jax import lax

MODEL_WIDTH = 4096
QUERY_HEADS = 16
KEY_VALUE_HEADS = 4
HEAD_SIZE = 128
NDOC = 16
PACK_TOKENS = 4096
BLOCK_TOKENS = 512
DOC_MAX = 1024
REACH = 2


def shared_weights(key):
    expand_heads = MODEL_WIDTH ** (-0.5)
    base_query = jax.random.truncated_normal(jax.random.fold_in(key, 11), -6.0, 6.0, (MODEL_WIDTH, QUERY_HEADS, HEAD_SIZE), jnp.float32) * expand_heads
    unrotated_keys = jax.random.truncated_normal(jax.random.fold_in(key, 12), -6.0, 6.0, (MODEL_WIDTH, KEY_VALUE_HEADS, HEAD_SIZE), jnp.float32) * expand_heads
    projected_values = jax.random.truncated_normal(jax.random.fold_in(key, 13), -6.0, 6.0, (MODEL_WIDTH, KEY_VALUE_HEADS, HEAD_SIZE), jnp.float32) * expand_heads
    key_matrix = unrotated_keys
    query_weights = base_query
    limit = 48.0 * expand_heads
    query_weights = jnp.clip(query_weights, -limit, limit).reshape(MODEL_WIDTH, QUERY_HEADS * HEAD_SIZE)
    key_value_matrix = jnp.stack([key_matrix.reshape(MODEL_WIDTH, KEY_VALUE_HEADS * HEAD_SIZE), projected_values.reshape(MODEL_WIDTH, KEY_VALUE_HEADS * HEAD_SIZE)], axis=1)
    key_value_matrix = jnp.clip(key_value_matrix, -limit, limit)
    return (query_weights, key_value_matrix)


def draw_w_query(key, part):
    return shared_weights(key)[0].astype(jnp.bfloat16)


def draw_key_value_weight(key, part):
    return shared_weights(key)[1].astype(jnp.bfloat16)


def draw_tokens(key, part):
    own_part = jax.random.normal(jax.random.fold_in(key, 21), (PACK_TOKENS, MODEL_WIDTH), jnp.float32)
    result = own_part
    return jnp.clip(result, -6.0, 6.0).astype(jnp.bfloat16)


def block_scale(own_key, dims, cuts, low, high):
    loudness = 1.0
    for position, blocks in cuts:
        steps = jax.random.uniform(jax.random.fold_in(jax.random.fold_in(own_key, 6), position), (blocks,), jnp.float32, low / len(cuts), high / len(cuts))
        loudness = loudness * jnp.repeat(jnp.exp(steps), dims[position] // blocks).reshape((-1,) + (1,) * (len(dims) - 1 - position))
    return loudness


def split_up(count, total, most, slope):
    weights = [(1 << 20) // math.isqrt(rank ** slope) + 1 for rank in range(2, count + 1)]
    surplus, holding = total - most - (count - 1), [1] * (count - 1)
    while surplus > 0:
        movable = [i for i in range(count - 1) if holding[i] < most]
        pool, budget = sum([weights[i] for i in movable]), surplus
        for i in movable:
            more = min(most - holding[i], max(1, budget * weights[i] // pool), surplus)
            holding[i] = holding[i] + more
            surplus = surplus - more
    return np.array([most] + holding)


def ragged_sizes(key, amount, total, most, slope):
    if amount == 2:
        one = jax.random.randint(key, (), max(1, total - most), min(most, total - 1) + 1)
        return jnp.stack([one, total - one])
    sizes = jnp.asarray(split_up(amount, total, most, slope), jnp.int32)
    twos = (amount - 1) // 2
    source_of, sink = sizes[1:1 + 2 * twos:2], sizes[2:2 + 2 * twos:2]
    room = jnp.minimum(source_of - 1, most - sink)
    passed = jax.random.randint(jax.random.fold_in(key, 1), (twos,), 0, 1 << 20) % (room + 1)
    sizes = sizes.at[1:1 + 2 * twos:2].set(source_of - passed).at[2:2 + 2 * twos:2].set(sink + passed)
    return sizes[jax.random.permutation(jax.random.fold_in(key, 2), amount)]


def scatter_about(stream_key, shape, scale, most, split=(), kind=jnp.bfloat16):
    values = jax.random.normal(stream_key, shape, jnp.float32) * scale
    if len(split) > 0:
        values = block_scale(stream_key, shape, split, -0.22, 0.18) * values
    return jnp.clip(values, min=-most, max=most).astype(kind)


def setup_inputs(seed: int = 0) -> dict:
    keys = jax.random.split(jax.random.key(seed), 6)
    return {
        "tokens": draw_tokens(jax.random.fold_in(keys[5], 71), 0),
        "w_query": draw_w_query(jax.random.fold_in(keys[5], 71), 0),
        "key_value_weight": draw_key_value_weight(jax.random.fold_in(keys[5], 71), 0),
        "w_out": scatter_about(keys[3], (QUERY_HEADS * HEAD_SIZE, MODEL_WIDTH), HEAD_SIZE ** -0.5, 0.5, ((0, 32),)),
        "doc_lengths": ragged_sizes(keys[4], NDOC, PACK_TOKENS, DOC_MAX, 2).astype(jnp.int32),
    }


norm_epsilon = 1e-05
rope_base = 500000.0
masked_score = -1e+30

def locate_documents(positions, doc_lengths):
    ends = jnp.cumsum(doc_lengths).astype(jnp.int32)
    after = positions[:, None] >= ends[None, :]
    ident = lax.optimization_barrier(jnp.sum(after.astype(jnp.int32), axis=1))
    starts = lax.optimization_barrier(jnp.sum(jnp.where(after, doc_lengths[None, :], 0), axis=1)).astype(jnp.int32)
    return (ident, starts)

def apply_rotation(values, relative_offset):
    half = values.shape[-1] // 2
    freqs = jnp.power(rope_base, -2.0 * jnp.arange(half, dtype=jnp.float32) / values.shape[-1])
    angle = relative_offset.astype(jnp.float32)[:, None] * freqs[None, :]
    cosine = jnp.cos(angle)[:, None, :]
    sine = jnp.sin(angle)[:, None, :]
    first = values[..., :half]
    second = values[..., half:]
    return jnp.concatenate([first * cosine - second * sine, second * cosine + first * sine], axis=-1)

def reference(tokens, w_query, key_value_weight, w_out, doc_lengths):
    values = tokens.astype(jnp.float32)
    normalized_input = (values * lax.rsqrt(lax.optimization_barrier(jnp.mean(values * values, axis=1, keepdims=True)) + norm_epsilon)).astype(jnp.bfloat16)
    query_raw = jnp.dot(normalized_input, w_query, preferred_element_type=jnp.float32)
    key_value_projected = jnp.dot(normalized_input, key_value_weight.reshape(MODEL_WIDTH, 2 * KEY_VALUE_HEADS * HEAD_SIZE), preferred_element_type=jnp.float32)
    positions = jnp.arange(PACK_TOKENS, dtype=jnp.int32)
    ident, starts = locate_documents(positions, doc_lengths)
    relative_offset = positions - starts
    query_rows = apply_rotation(query_raw.reshape(PACK_TOKENS, QUERY_HEADS, HEAD_SIZE), relative_offset).astype(jnp.bfloat16)
    rotated_keys = apply_rotation(key_value_projected[:, :KEY_VALUE_HEADS * HEAD_SIZE].reshape(PACK_TOKENS, KEY_VALUE_HEADS, HEAD_SIZE), relative_offset).astype(jnp.bfloat16)
    value_rows = key_value_projected[:, KEY_VALUE_HEADS * HEAD_SIZE:].reshape(PACK_TOKENS, KEY_VALUE_HEADS, HEAD_SIZE).astype(jnp.bfloat16)
    front_offset = REACH * BLOCK_TOKENS
    window = (REACH + 1) * BLOCK_TOKENS
    padded_key_rows = jnp.concatenate([jnp.zeros((front_offset, KEY_VALUE_HEADS, HEAD_SIZE), jnp.bfloat16), rotated_keys], axis=0)
    padded_value_rows = jnp.concatenate([jnp.zeros((front_offset, KEY_VALUE_HEADS, HEAD_SIZE), jnp.bfloat16), value_rows], axis=0)
    head_group = QUERY_HEADS // KEY_VALUE_HEADS
    scale = HEAD_SIZE ** (-0.5)

    def one_block(block_index):
        leading_row = (block_index * BLOCK_TOKENS).astype(jnp.int32)
        query_block_rows = lax.dynamic_slice_in_dim(query_rows, leading_row, BLOCK_TOKENS, 0).reshape(BLOCK_TOKENS, KEY_VALUE_HEADS, head_group, HEAD_SIZE).astype(jnp.float32)
        key_block = lax.dynamic_slice_in_dim(padded_key_rows, leading_row, window, 0).astype(jnp.float32)
        value_block = lax.dynamic_slice_in_dim(padded_value_rows, leading_row, window, 0).astype(jnp.float32)
        query_pos = leading_row + jnp.arange(BLOCK_TOKENS, dtype=jnp.int32)
        key_pos = leading_row - front_offset + jnp.arange(window, dtype=jnp.int32)
        query_doc, unused_q = locate_documents(query_pos, doc_lengths)
        key_doc, unused_k = locate_documents(key_pos, doc_lengths)
        keep = (key_pos[None, :] >= 0) & (key_pos[None, :] <= query_pos[:, None]) & (key_doc[None, :] == query_doc[:, None])
        scores = jnp.einsum('qhgd,khd->hgqk', query_block_rows, key_block) * scale
        scores = jnp.where(keep, scores, masked_score)
        highest = lax.optimization_barrier(jnp.max(scores, axis=-1, keepdims=True))
        probs = jnp.where(keep, jnp.exp(scores - highest), 0.0)
        totals = lax.optimization_barrier(jnp.sum(probs, axis=-1))
        probs_b = lax.optimization_barrier(probs.astype(jnp.bfloat16))
        mixed = jnp.einsum('hgqk,khd->hgqd', probs_b.astype(jnp.float32), value_block)
        mixed = mixed / totals[..., None]
        return mixed.transpose(2, 0, 1, 3).reshape(BLOCK_TOKENS, QUERY_HEADS * HEAD_SIZE).astype(jnp.bfloat16)
    mixed_all = lax.map(one_block, jnp.arange(PACK_TOKENS // BLOCK_TOKENS, dtype=jnp.int32)).reshape(PACK_TOKENS, QUERY_HEADS * HEAD_SIZE)
    return jnp.dot(mixed_all, w_out, preferred_element_type=jnp.float32).astype(jnp.bfloat16)
```

```python
import functools

import jax
import jax.numpy as jnp
from jax import lax
from jax.experimental import pallas as pl
from jax.experimental.pallas import tpu as pltpu
from jax.sharding import PartitionSpec as P

HEAD_SIZE = 128
CHUNKS = 2
LINE = 2

norm_epsilon = 1e-05
rope_base = 500000.0
masked_score = -1e30
MESH = pl.DeviceIdType.MESH
UP, DOWN, ACROSS = 0, 1, 2


def layer_kernel(
    n, heads, chunks,
    tok_ref, w_in_ref, w_out_ref, len_ref, freq_ref, out_ref,
    w_in, w_proj, acts, qkv, query, kv, high, total, accum, mixed, rope,
    near_send, near_recv, part, far_send, far_recv,
    local_sem, in_send, in_recv, proj_send, proj_recv, bal_send,
    act_send, act_recv, kv_send, kv_recv, near_ss, near_rs, far_ss, far_rs,
):
    f32, bf16 = jnp.float32, jnp.bfloat16
    b = lax.axis_index("blk")
    h = lax.axis_index("heads")
    steps = n // LINE
    z, x = b // LINE, b % LINE
    outer = heads // 2
    y, core = h // 2, h % 2
    mate = y * 2 + 1 - core
    reach = n // 4
    tokens_own, width = tok_ref.shape
    rows_in, in_cols = w_in_ref.shape
    rows_out = w_out_ref.shape[0]
    chunk_cols = w_out_ref.shape[1] // chunks
    block = tokens_own * heads
    q_cols = query.shape[1]
    q_heads = q_cols // HEAD_SIZE

    def at_blk(i):
        return {"blk": i}

    def at_head(i):
        return {"heads": i}

    def remote(src, dst, ss, rs, dev):
        return pltpu.make_async_remote_copy(
            src_ref=src, dst_ref=dst, send_sem=ss, recv_sem=rs, device_id=dev, device_id_type=MESH
        )

    barrier = pltpu.get_barrier_semaphore()
    span = max(reach, LINE)
    peers = 0
    for d in sorted({e % n for k in range(1, span + 1) for e in (k, -k)}):
        pl.semaphore_signal(barrier, inc=1, device_id=at_blk(lax.rem(b + d, n)), device_id_type=MESH)
        peers += 1
    for d in range(1, heads):
        pl.semaphore_signal(barrier, inc=1, device_id=at_head(lax.rem(h + d, heads)), device_id_type=MESH)
        peers += 1
    pl.semaphore_wait(barrier, peers)

    def in_slot(i):
        return w_in.at[pl.ds(pl.multiple_of(i * rows_in, rows_in), rows_in)]

    def proj_slot(c, i):
        return w_proj.at[c, i]

    def proj_own(c):
        return w_out_ref.at[:, pl.ds(c * chunk_cols, chunk_cols)]

    def stream(c):
        if c < 0:
            return in_slot, w_in_ref, lambda d, r: in_send.at[d, r], lambda i: in_recv.at[i]
        return (
            functools.partial(proj_slot, c), proj_own(c),
            lambda d, r: proj_send.at[c, d, r], lambda i: proj_recv.at[c, i],
        )

    def target(direction):
        if direction == UP:
            return at_blk(lax.rem(b + LINE, n))
        if direction == DOWN:
            return at_blk(lax.rem(b + n - LINE, n))
        return at_blk(z * LINE + 1 - x)

    def send_copy(c, direction, row, own):
        slot, source, ss, rs = stream(c)
        origin = row * LINE + x
        dst = slot(origin)
        return remote(source if own else dst, dst, ss(direction, row), rs(origin), target(direction))

    def await_slot(c, origin):
        slot, source, ss, rs = stream(c)
        ref = slot(origin)
        remote(ref, ref, ss(0, 0), rs(origin), target(ACROSS)).wait_recv()

    def crosses(c, row):
        if c < 0:
            return row >= 0
        return jnp.logical_not(((z == 0) & (row == 1)) | ((z == steps - 1) & (row == steps - 2)))

    def line_own(c):
        @pl.when(z < steps - 1)
        def _():
            send_copy(c, UP, z, True).start()

        @pl.when(z > 0)
        def _():
            send_copy(c, DOWN, z, True).start()

    def line_step(c, s):
        @pl.when(z - s >= 0)
        def _():
            await_slot(c, (z - s) * LINE + x)

            @pl.when(z < steps - 1)
            def _():
                send_copy(c, UP, z - s, False).start()

        @pl.when(z + s <= steps - 1)
        def _():
            await_slot(c, (z + s) * LINE + x)

            @pl.when(z > 0)
            def _():
                send_copy(c, DOWN, z + s, False).start()

    def cross_own(c):
        send_copy(c, ACROSS, z, True).start()

    def cross_step(c, s):
        @pl.when((z - s >= 0) & crosses(c, z - s))
        def _():
            send_copy(c, ACROSS, z - s, False).start()

        @pl.when((z + s <= steps - 1) & crosses(c, z + s))
        def _():
            send_copy(c, ACROSS, z + s, False).start()

    def side_copy(c, end):
        ref = proj_slot(c, z * LINE + 1 - x)
        return remote(ref, ref, bal_send.at[c, end], proj_recv.at[c, z * LINE + 1 - x],
                      target(DOWN if end == 0 else UP))

    def balance(c):
        @pl.when((z == 1) | (z == steps - 2))
        def _():
            await_slot(c, z * LINE + 1 - x)

        @pl.when(z == 1)
        def _():
            side_copy(c, 0).start()

        @pl.when(z == steps - 2)
        def _():
            side_copy(c, 1).start()

    def await_crossed(c):
        def one(row, _):
            already = ((z == 1) | (z == steps - 2)) & (row == z) & (c >= 0)

            @pl.when(jnp.logical_not(already))
            def _():
                await_slot(c, row * LINE + 1 - x)
            return 0

        lax.fori_loop(0, steps, one, 0)

    line_own(-1)
    cross_own(-1)
    keep_in = pltpu.make_async_copy(w_in_ref, in_slot(b), local_sem.at[chunks])
    keep_in.start()
    keep_out = [
        pltpu.make_async_copy(proj_own(c), proj_slot(c, b), local_sem.at[c]) for c in range(chunks)
    ]
    for copy in keep_out:
        copy.start()

    values = tok_ref[...].astype(f32)
    acts[h] = (
        values * lax.rsqrt(jnp.mean(values * values, axis=1, keepdims=True) + norm_epsilon)
    ).astype(bf16)

    act_copies = []
    for o in range(1, outer):
        act_copies.append(remote(acts.at[h], acts.at[h], act_send.at[o], act_recv.at[h],
                                 at_head(lax.rem(y + o, outer) * 2 + core)))
    act_copies.append(remote(acts.at[h], acts.at[h], act_send.at[0], act_recv.at[h], at_head(mate)))
    for copy in act_copies:
        copy.start()

    pos = b * block + lax.broadcasted_iota(jnp.int32, (block, 1), 0)
    start = jnp.zeros((block, 1), jnp.int32)
    end = jnp.int32(0)
    for i in range(len_ref.shape[0]):
        size = len_ref[i]
        end = end + size
        start = start + jnp.where(pos >= end, size, 0)
    angle = (pos - start).astype(f32) * freq_ref[...]
    lane = lax.broadcasted_iota(jnp.int32, (block, HEAD_SIZE), 1)
    rope[0] = jnp.cos(angle)
    rope[1] = jnp.where(lane < HEAD_SIZE // 2, -jnp.sin(angle), jnp.sin(angle))

    def in_step(s, _):
        line_step(-1, s)
        cross_step(-1, s)
        return 0

    in_step(1, 0)
    for o in range(1, outer):
        other = lax.rem(y + o, outer) * 2 + core
        remote(acts.at[other], acts.at[other], act_send.at[0], act_recv.at[other], at_head(mate)).wait_recv()
        copy = remote(acts.at[other], acts.at[other], act_send.at[outer + o], act_recv.at[other], at_head(mate))
        copy.start()
        act_copies.append(copy)
    lax.fori_loop(2, steps, in_step, 0)

    for c in range(chunks):
        line_own(c)
    cross_own(0)
    line_events = [(c, s) for s in range(1, steps) for c in range(chunks)]

    def run_events(count):
        for _ in range(min(count, len(line_events))):
            c, s = line_events.pop(0)
            line_step(c, s)
            if c == 0:
                cross_step(0, s)

    run_events(2 * chunks - 1)

    keep_in.wait()
    await_crossed(-1)
    for o in range(outer):
        other = lax.rem(y + o, outer) * 2 + 1 - core
        remote(acts.at[other], acts.at[other], act_send.at[0], act_recv.at[other], at_head(mate)).wait_recv()

    depth = min(512, width)

    def project(k, _):
        cols = pl.ds(pl.multiple_of(k * depth, depth), depth)
        left = acts[:, :, cols].reshape(block, depth)
        term = jnp.dot(left, w_in[cols, :], preferred_element_type=f32)
        qkv[...] = term + qkv[...]
        return 0

    qkv[...] = jnp.zeros_like(qkv)
    lax.fori_loop(0, width // depth, project, 0)

    cosine, sine = rope[0], rope[1]

    def rotated(first):
        v = qkv[:, first:first + HEAD_SIZE]
        return (v * cosine + pltpu.roll(v, HEAD_SIZE // 2, 1) * sine).astype(bf16)

    kv[0, :, :HEAD_SIZE] = rotated(q_cols)
    kv[0, :, HEAD_SIZE:] = qkv[:, q_cols + HEAD_SIZE:].astype(bf16)
    for j in range(q_heads):
        query[:, j * HEAD_SIZE:(j + 1) * HEAD_SIZE] = rotated(j * HEAD_SIZE)

    def kv_copy(d):
        return remote(kv.at[0], kv.at[d], kv_send.at[d], kv_recv.at[d], at_blk(lax.rem(b + d, n)))

    def kv_start(d, _):
        @pl.when(b + d < n)
        def _():
            kv_copy(d).start()
        return 0

    lax.fori_loop(1, reach + 1, kv_start, 0)
    run_events(chunks)

    scale = HEAD_SIZE ** (-0.5)
    high[...] = jnp.full_like(high, masked_score)
    total[...] = jnp.zeros_like(total)
    accum[...] = jnp.zeros_like(accum)
    own_pos = lax.broadcasted_iota(jnp.int32, (block, 1), 0)
    own_start = start - b * block
    key_lane = lax.broadcasted_iota(jnp.int32, (1, block), 1)

    def attend(d):
        key_pos = key_lane - d * block
        keep = (key_pos >= own_start) & (key_pos <= own_pos)

        def one(j, _):
            cols = pl.ds(pl.multiple_of(j * HEAD_SIZE, HEAD_SIZE), HEAD_SIZE)
            scores = lax.dot_general(
                query[:, cols], kv[d, :, :HEAD_SIZE], (((1,), (1,)), ((), ())),
                preferred_element_type=f32,
            ) * scale
            scores = jnp.where(keep, scores, masked_score)
            old = high[j]
            new = jnp.maximum(old, jnp.max(scores, axis=1, keepdims=True))
            fading = jnp.exp(old - new)
            probs = jnp.where(keep, jnp.exp(scores - new), 0.0)
            total[j] = total[j] * fading + jnp.sum(probs, axis=1, keepdims=True)
            update = jnp.dot(probs.astype(bf16), kv[d, :, HEAD_SIZE:], preferred_element_type=f32)
            accum[:, cols] = accum[:, cols] * fading + update
            high[j] = new
            return 0

        lax.fori_loop(0, q_heads, one, 0)

    attend(0)
    run_events(len(line_events))
    balance(0)
    for c in range(1, chunks):
        cross_own(c)
        for s in range(1, steps):
            cross_step(c, s)

    def earlier(d, _):
        @pl.when(b >= d)
        def _():
            remote(kv.at[d], kv.at[d], kv_send.at[d], kv_recv.at[d], at_blk(lax.rem(b + 1, n))).wait_recv()
            attend(d)
        return 0

    lax.fori_loop(1, reach + 1, earlier, 0)

    for g in range(heads):
        rows = slice(g * tokens_own, (g + 1) * tokens_own)
        for j in range(q_heads):
            cols = slice(j * HEAD_SIZE, (j + 1) * HEAD_SIZE)
            mixed[g % 2, g // 2, :, cols] = (accum[rows, cols] / total[j, rows]).astype(bf16)

    tile = min(512, chunk_cols)

    def weight_tile(c, cols):
        right = w_proj[c, :, :, cols]
        if rows_out % 16:
            return right.astype(f32).reshape(n * rows_out, tile).astype(bf16)
        return right.reshape(n * rows_out, tile)

    def near_copy(c):
        return remote(near_send.at[c], near_recv.at[c], near_ss.at[c], near_rs.at[c], at_head(mate))

    def far_copy(c, o):
        other = lax.rem(y + o, outer)
        return remote(far_send.at[c, o], far_recv.at[c, o], far_ss.at[c, o], far_rs.at[c, o],
                      at_head(other * 2 + core))

    def project_out(c):
        keep_out[c].wait()
        await_crossed(c)

        def theirs(k, _):
            cols = pl.ds(pl.multiple_of(k * tile, tile), tile)
            left = mixed[1 - core].reshape(outer * tokens_own, q_cols)
            term = jnp.dot(left, weight_tile(c, cols), preferred_element_type=f32)
            near_send[c, :, :, cols] = term.astype(bf16).reshape(outer, tokens_own, tile)
            return 0

        def ours(k, _):
            cols = pl.ds(pl.multiple_of(k * tile, tile), tile)
            left = mixed[core].reshape(outer * tokens_own, q_cols)
            term = jnp.dot(left, weight_tile(c, cols), preferred_element_type=f32)
            part[c, :, :, cols] = term.reshape(outer, tokens_own, tile)
            return 0

        lax.fori_loop(0, chunk_cols // tile, theirs, 0)
        near_copy(c).start()
        lax.fori_loop(0, chunk_cols // tile, ours, 0)
        near_copy(c).wait_recv()
        for o in range(1, outer):
            other = lax.rem(y + o, outer)
            far_send[c, o] = (part[c, other] + near_recv[c, other].astype(f32)).astype(bf16)
            far_copy(c, o).start()

    def finish(c):
        result = part[c, y] + near_recv[c, y].astype(f32)
        for o in range(1, outer):
            far_copy(c, o).wait_recv()
            result = result + far_recv[c, o].astype(f32)
        out_ref[:, c * chunk_cols:(c + 1) * chunk_cols] = result.astype(bf16)

    for c in range(chunks):
        project_out(c)
        if c + 1 < chunks:
            balance(c + 1)
        if c > 0:
            finish(c - 1)
    finish(chunks - 1)

    def drain(c):
        def one(row, _):
            @pl.when((row <= z) & (z < steps - 1))
            def _():
                send_copy(c, UP, row, False).wait_send()

            @pl.when((row >= z) & (z > 0))
            def _():
                send_copy(c, DOWN, row, False).wait_send()

            @pl.when(crosses(c, row))
            def _():
                send_copy(c, ACROSS, row, False).wait_send()
            return 0

        lax.fori_loop(0, steps, one, 0)

    for c in range(-1, chunks):
        drain(c)
    for c in range(chunks):
        @pl.when(z == 1)
        def _():
            side_copy(c, 0).wait_send()

        @pl.when(z == steps - 2)
        def _():
            side_copy(c, 1).wait_send()

        near_copy(c).wait_send()
        for o in range(1, outer):
            far_copy(c, o).wait_send()
    for copy in act_copies:
        copy.wait_send()

    def kv_drain(d, _):
        @pl.when(b + d < n)
        def _():
            kv_copy(d).wait_send()
        return 0

    lax.fori_loop(1, reach + 1, kv_drain, 0)


def on_device(tokens, w_query, key_value_weight, w_out, doc_lengths):
    n = lax.axis_size("blk")
    heads = lax.axis_size("heads")
    chunks = CHUNKS
    outer = heads // 2
    steps = n // LINE
    own, width = tokens.shape
    block = own * heads
    rows_in, q_cols = w_query.shape
    kv_cols = 2 * key_value_weight.shape[2]
    rows_out = w_out.shape[0]
    chunk_cols = width // chunks
    q_heads = q_cols // HEAD_SIZE
    reach = n // 4
    w_in = jnp.concatenate([w_query, key_value_weight.reshape(rows_in, kv_cols)], axis=1)
    half = HEAD_SIZE // 2
    freqs = jnp.power(rope_base, -2.0 * jnp.arange(half, dtype=jnp.float32) / HEAD_SIZE)
    freqs = jnp.concatenate([freqs, freqs])[None, :]
    bf16, f32 = jnp.bfloat16, jnp.float32
    dma = pltpu.SemaphoreType.DMA
    return pl.pallas_call(
        functools.partial(layer_kernel, n, heads, chunks),
        out_shape=jax.ShapeDtypeStruct((own, width), bf16),
        in_specs=[
            pl.BlockSpec(memory_space=pltpu.VMEM),
            pl.BlockSpec(memory_space=pl.ANY),
            pl.BlockSpec(memory_space=pl.ANY),
            pl.BlockSpec(memory_space=pltpu.SMEM),
            pl.BlockSpec(memory_space=pltpu.VMEM),
        ],
        out_specs=pl.BlockSpec(memory_space=pltpu.VMEM),
        scratch_shapes=[
            pltpu.VMEM((n * rows_in, q_cols + kv_cols), bf16),
            pltpu.VMEM((chunks, n, rows_out, chunk_cols), bf16),
            pltpu.VMEM((heads, own, width), bf16),
            pltpu.VMEM((block, q_cols + kv_cols), f32),
            pltpu.VMEM((block, q_cols), bf16),
            pltpu.VMEM((reach + 1, block, kv_cols), bf16),
            pltpu.VMEM((q_heads, block, 1), f32),
            pltpu.VMEM((q_heads, block, 1), f32),
            pltpu.VMEM((block, q_cols), f32),
            pltpu.VMEM((2, outer, own, q_cols), bf16),
            pltpu.VMEM((2, block, HEAD_SIZE), f32),
            pltpu.VMEM((chunks, outer, own, chunk_cols), bf16),
            pltpu.VMEM((chunks, outer, own, chunk_cols), bf16),
            pltpu.VMEM((chunks, outer, own, chunk_cols), f32),
            pltpu.VMEM((chunks, outer, own, chunk_cols), bf16),
            pltpu.VMEM((chunks, outer, own, chunk_cols), bf16),
            dma((chunks + 1,)),
            dma((3, steps)),
            dma((n,)),
            dma((chunks, 3, steps)),
            dma((chunks, n)),
            dma((chunks, 2)),
            dma((2 * outer,)),
            dma((heads,)),
            dma((reach + 1,)),
            dma((reach + 1,)),
            dma((chunks,)),
            dma((chunks,)),
            dma((chunks, outer)),
            dma((chunks, outer)),
        ],
        compiler_params=pltpu.CompilerParams(
            collective_id=0, has_side_effects=True, vmem_limit_bytes=60 * 1024 * 1024
        ),
    )(tokens, w_in, w_out, doc_lengths, freqs)


def solution(mesh):
    return jax.shard_map(
        on_device,
        mesh=mesh,
        in_specs=(
            P(("blk", "heads"), None),
            P("blk", "heads"),
            P("blk", None, "heads"),
            P(("heads", "blk"), None),
            P(),
        ),
        out_specs=P(("blk", "heads"), None),
        check_vma=False,
    )
```

```python
import functools

import jax
import jax.numpy as jnp
import numpy as np
from jax import lax
from jax.experimental import pallas as pl
from jax.experimental.pallas import tpu as pltpu
from jax.sharding import PartitionSpec as P

HEAD_SIZE = 128
CHUNKS = 4
LINE = 2

norm_epsilon = 1e-05
rope_base = 500000.0
masked_score = -1e30
MESH = pl.DeviceIdType.MESH
UP, DOWN, ACROSS = 0, 1, 2
QUERY, KEYVAL = -1, -2


def layer_kernel(
    n, heads, chunks,
    tok_ref, w_query_ref, w_keyval_ref, w_out_ref, len_ref, freq_ref, out_ref,
    w_in, w_kv, w_proj, acts, qkv, query, kv, high, total, accum, mixed, rope,
    near_send, near_recv, part, far_send, far_recv,
    local_sem, in_send, in_recv, proj_send, proj_recv, bal_send,
    act_send, act_recv, kv_send, kv_recv, near_ss, near_rs, far_ss, far_rs,
):
    f32, bf16 = jnp.float32, jnp.bfloat16
    b = lax.axis_index("blk")
    h = lax.axis_index("heads")
    steps = n // LINE
    z, x = b // LINE, b % LINE
    outer = heads // 2
    y, core = h // 2, h % 2
    mate = y * 2 + 1 - core
    reach = n // 4
    tokens_own, width = tok_ref.shape
    rows_in = w_query_ref.shape[0]
    rows_out = w_out_ref.shape[0]
    chunk_cols = w_out_ref.shape[1] // chunks
    block = tokens_own * heads
    q_cols = query.shape[1]
    q_heads = q_cols // HEAD_SIZE

    def at_blk(i):
        return {"blk": i}

    def at_head(i):
        return {"heads": i}

    def remote(src, dst, ss, rs, dev):
        return pltpu.make_async_remote_copy(
            src_ref=src, dst_ref=dst, send_sem=ss, recv_sem=rs, device_id=dev, device_id_type=MESH
        )

    barrier = pltpu.get_barrier_semaphore()
    span = max(reach, LINE)
    peers = 0
    for d in sorted({e % n for k in range(1, span + 1) for e in (k, -k)}):
        pl.semaphore_signal(barrier, inc=1, device_id=at_blk(lax.rem(b + d, n)), device_id_type=MESH)
        peers += 1
    for d in range(1, heads):
        pl.semaphore_signal(barrier, inc=1, device_id=at_head(lax.rem(h + d, heads)), device_id_type=MESH)
        peers += 1
    pl.semaphore_wait(barrier, peers)

    def in_slot(i):
        return w_in.at[pl.ds(pl.multiple_of(i * rows_in, rows_in), rows_in)]

    def kv_slot(i):
        return w_kv.at[pl.ds(pl.multiple_of(i * rows_in, rows_in), rows_in)]

    def proj_slot(c, i):
        return w_proj.at[c, i]

    def proj_own(c):
        return w_out_ref.at[:, pl.ds(c * chunk_cols, chunk_cols)]

    def stream(c):
        if c < 0:
            slot, source = (in_slot, w_query_ref) if c == QUERY else (kv_slot, kv_slot(b))
            return slot, source, lambda d, r: in_send.at[c + 2, d, r], lambda i: in_recv.at[c + 2, i]
        return (
            functools.partial(proj_slot, c), proj_own(c),
            lambda d, r: proj_send.at[c, d, r], lambda i: proj_recv.at[c, i],
        )

    def target(direction):
        if direction == UP:
            return at_blk(lax.rem(b + LINE, n))
        if direction == DOWN:
            return at_blk(lax.rem(b + n - LINE, n))
        return at_blk(z * LINE + 1 - x)

    def send_copy(c, direction, row, own):
        slot, source, ss, rs = stream(c)
        origin = row * LINE + x
        dst = slot(origin)
        return remote(source if own else dst, dst, ss(direction, row), rs(origin), target(direction))

    def await_slot(c, origin):
        slot, source, ss, rs = stream(c)
        ref = slot(origin)
        remote(ref, ref, ss(0, 0), rs(origin), target(ACROSS)).wait_recv()

    twin = z + 1 - 2 * (z % 2)

    def crosses(c, row):
        if c < 0:
            return row >= 0
        return row != twin

    def line_own(c):
        @pl.when(z < steps - 1)
        def _():
            send_copy(c, UP, z, True).start()

        @pl.when(z > 0)
        def _():
            send_copy(c, DOWN, z, True).start()

    def line_step(c, s):
        @pl.when(z - s >= 0)
        def _():
            await_slot(c, (z - s) * LINE + x)

            @pl.when(z < steps - 1)
            def _():
                send_copy(c, UP, z - s, False).start()

        @pl.when(z + s <= steps - 1)
        def _():
            await_slot(c, (z + s) * LINE + x)

            @pl.when(z > 0)
            def _():
                send_copy(c, DOWN, z + s, False).start()

    def cross_own(c):
        send_copy(c, ACROSS, z, True).start()

    def cross_step(c, s):
        @pl.when((z - s >= 0) & crosses(c, z - s))
        def _():
            send_copy(c, ACROSS, z - s, False).start()

        @pl.when((z + s <= steps - 1) & crosses(c, z + s))
        def _():
            send_copy(c, ACROSS, z + s, False).start()

    def side_copy(c):
        ref = proj_slot(c, z * LINE + 1 - x)
        return remote(ref, ref, bal_send.at[c], proj_recv.at[c, z * LINE + 1 - x],
                      at_blk(twin * LINE + x))

    def balance(c):
        @pl.when(twin < steps)
        def _():
            await_slot(c, z * LINE + 1 - x)
            side_copy(c).start()

    def await_crossed(c):
        def one(row, _):
            if c < 0:
                await_slot(c, row * LINE + 1 - x)
            else:
                @pl.when((row != z) | (twin >= steps))
                def _():
                    await_slot(c, row * LINE + 1 - x)
            return 0

        lax.fori_loop(0, steps, one, 0)

    line_own(QUERY)
    cross_own(QUERY)
    keep_in = pltpu.make_async_copy(w_query_ref, in_slot(b), local_sem.at[chunks])
    keep_in.start()
    w_kv[pl.ds(pl.multiple_of(b * rows_in, rows_in), rows_in), :] = w_keyval_ref[...].reshape(
        rows_in, w_kv.shape[1]
    )
    line_own(KEYVAL)
    cross_own(KEYVAL)
    keep_out = [
        pltpu.make_async_copy(proj_own(c), proj_slot(c, b), local_sem.at[c]) for c in range(chunks)
    ]
    for copy in keep_out:
        copy.start()

    values = tok_ref[...].astype(f32)
    acts[h] = (
        values * lax.rsqrt(jnp.mean(values * values, axis=1, keepdims=True) + norm_epsilon)
    ).astype(bf16)

    act_copies = []
    for o in range(1, outer):
        act_copies.append(remote(acts.at[h], acts.at[h], act_send.at[o], act_recv.at[h],
                                 at_head(lax.rem(y + o, outer) * 2 + core)))
    act_copies.append(remote(acts.at[h], acts.at[h], act_send.at[0], act_recv.at[h], at_head(mate)))
    for copy in act_copies:
        copy.start()

    pos = b * block + lax.broadcasted_iota(jnp.int32, (block, 1), 0)
    start = jnp.zeros((block, 1), jnp.int32)
    end = jnp.int32(0)
    for i in range(len_ref.shape[0]):
        size = len_ref[i]
        end = end + size
        start = start + jnp.where(pos >= end, size, 0)
    angle = (pos - start).astype(f32) * freq_ref[...]
    lane = lax.broadcasted_iota(jnp.int32, (block, HEAD_SIZE), 1)
    rope[0] = jnp.cos(angle)
    rope[1] = jnp.where(lane < HEAD_SIZE // 2, -jnp.sin(angle), jnp.sin(angle))

    def in_step(s, _):
        for c in (QUERY, KEYVAL):
            line_step(c, s)
            cross_step(c, s)
        return 0

    in_step(1, 0)
    for o in range(1, outer):
        other = lax.rem(y + o, outer) * 2 + core
        remote(acts.at[other], acts.at[other], act_send.at[0], act_recv.at[other], at_head(mate)).wait_recv()
        copy = remote(acts.at[other], acts.at[other], act_send.at[outer + o], act_recv.at[other], at_head(mate))
        copy.start()
        act_copies.append(copy)
    lax.fori_loop(2, steps - 1, in_step, 0)

    for c in range(chunks):
        line_own(c)
    in_step(steps - 1, 0)
    for c in range(chunks // 2):
        cross_own(c)
    line_events = [(c, s) for s in range(1, steps) for c in range(chunks)]

    def run_events(count):
        for _ in range(min(count, len(line_events))):
            c, s = line_events.pop(0)
            line_step(c, s)

    run_events(chunks + chunks // 2)

    keep_in.wait()
    await_crossed(QUERY)
    await_crossed(KEYVAL)
    for o in range(outer):
        other = lax.rem(y + o, outer) * 2 + 1 - core
        remote(acts.at[other], acts.at[other], act_send.at[0], act_recv.at[other], at_head(mate)).wait_recv()

    depth = min(512, width)

    def project(k, _):
        cols = pl.ds(pl.multiple_of(k * depth, depth), depth)
        left = acts[:, :, cols].reshape(block, depth)
        qkv[:, :q_cols] += jnp.dot(left, w_in[cols, :], preferred_element_type=f32)
        qkv[:, q_cols:] += jnp.dot(left, w_kv[cols, :], preferred_element_type=f32)
        return 0

    qkv[...] = jnp.zeros_like(qkv)
    lax.fori_loop(0, width // depth, project, 0)

    cosine, sine = rope[0], rope[1]

    def rotated(first):
        v = qkv[:, first:first + HEAD_SIZE]
        return (v * cosine + pltpu.roll(v, HEAD_SIZE // 2, 1) * sine).astype(bf16)

    kv[0, :, :HEAD_SIZE] = rotated(q_cols)
    kv[0, :, HEAD_SIZE:] = qkv[:, q_cols + HEAD_SIZE:].astype(bf16)
    for j in range(q_heads):
        query[:, j * HEAD_SIZE:(j + 1) * HEAD_SIZE] = rotated(j * HEAD_SIZE)

    def kv_copy(d):
        return remote(kv.at[0], kv.at[d], kv_send.at[d], kv_recv.at[d], at_blk(lax.rem(b + d, n)))

    def kv_start(d, _):
        @pl.when(b + d < n)
        def _():
            kv_copy(d).start()
        return 0

    lax.fori_loop(1, reach + 1, kv_start, 0)
    run_events(chunks - chunks // 2)

    scale = HEAD_SIZE ** (-0.5)
    high[...] = jnp.full_like(high, masked_score)
    total[...] = jnp.zeros_like(total)
    accum[...] = jnp.zeros_like(accum)
    own_pos = lax.broadcasted_iota(jnp.int32, (block, 1), 0)
    own_start = start - b * block
    key_lane = lax.broadcasted_iota(jnp.int32, (1, block), 1)

    def attend(d):
        key_pos = key_lane - d * block
        keep = (key_pos >= own_start) & (key_pos <= own_pos)

        def one(j, _):
            cols = pl.ds(pl.multiple_of(j * HEAD_SIZE, HEAD_SIZE), HEAD_SIZE)
            scores = lax.dot_general(
                query[:, cols], kv[d, :, :HEAD_SIZE], (((1,), (1,)), ((), ())),
                preferred_element_type=f32,
            ) * scale
            scores = jnp.where(keep, scores, masked_score)
            old = high[j]
            new = jnp.maximum(old, jnp.max(scores, axis=1, keepdims=True))
            fading = jnp.exp(old - new)
            probs = jnp.where(keep, jnp.exp(scores - new), 0.0)
            total[j] = total[j] * fading + jnp.sum(probs, axis=1, keepdims=True)
            update = jnp.dot(probs.astype(bf16), kv[d, :, HEAD_SIZE:], preferred_element_type=f32)
            accum[:, cols] = accum[:, cols] * fading + update
            high[j] = new
            return 0

        lax.fori_loop(0, q_heads, one, 0)

    for c in range(chunks):
        if c >= chunks // 2:
            cross_own(c)
        for s in range(1, steps):
            if (c, s) in line_events:
                line_step(c, s)
            cross_step(c, s)
        if c == 0:
            attend(0)
    early = min(2, chunks)
    for c in range(early):
        balance(c)

    def earlier(d, _):
        @pl.when(b >= d)
        def _():
            remote(kv.at[d], kv.at[d], kv_send.at[d], kv_recv.at[d], at_blk(lax.rem(b + 1, n))).wait_recv()
            attend(d)
        return 0

    lax.fori_loop(1, reach + 1, earlier, 0)

    for g in range(heads):
        rows = slice(g * tokens_own, (g + 1) * tokens_own)
        for j in range(q_heads):
            cols = slice(j * HEAD_SIZE, (j + 1) * HEAD_SIZE)
            mixed[g % 2, g // 2, :, cols] = (accum[rows, cols] / total[j, rows]).astype(bf16)

    tile = min(512, chunk_cols)

    def weight_tile(c, cols):
        right = w_proj[c, :, :, cols]
        if rows_out % 16:
            return right.astype(f32).reshape(n * rows_out, tile).astype(bf16)
        return right.reshape(n * rows_out, tile)

    def near_copy(c):
        return remote(near_send.at[c], near_recv.at[c], near_ss.at[c], near_rs.at[c], at_head(mate))

    def far_copy(c, o):
        other = lax.rem(y + o, outer)
        return remote(far_send.at[c, o], far_recv.at[c, o], far_ss.at[c, o], far_rs.at[c, o],
                      at_head(other * 2 + core))

    def project_out(c):
        keep_out[c].wait()
        await_crossed(c)

        def theirs(k, _):
            cols = pl.ds(pl.multiple_of(k * tile, tile), tile)
            left = mixed[1 - core].reshape(outer * tokens_own, q_cols)
            term = jnp.dot(left, weight_tile(c, cols), preferred_element_type=f32)
            near_send[c, :, :, cols] = term.astype(bf16).reshape(outer, tokens_own, tile)
            return 0

        def ours(k, _):
            cols = pl.ds(pl.multiple_of(k * tile, tile), tile)
            left = mixed[core].reshape(outer * tokens_own, q_cols)
            term = jnp.dot(left, weight_tile(c, cols), preferred_element_type=f32)
            part[c, :, :, cols] = term.reshape(outer, tokens_own, tile)
            return 0

        lax.fori_loop(0, chunk_cols // tile, theirs, 0)
        near_copy(c).start()
        lax.fori_loop(0, chunk_cols // tile, ours, 0)
        near_copy(c).wait_recv()
        for o in range(1, outer):
            other = lax.rem(y + o, outer)
            far_send[c, o] = (part[c, other] + near_recv[c, other].astype(f32)).astype(bf16)
            far_copy(c, o).start()

    def finish(c):
        result = part[c, y] + near_recv[c, y].astype(f32)
        for o in range(1, outer):
            far_copy(c, o).wait_recv()
            result = result + far_recv[c, o].astype(f32)
        out_ref[:, c * chunk_cols:(c + 1) * chunk_cols] = result.astype(bf16)

    for c in range(chunks):
        project_out(c)
        if early <= c + 1 < chunks:
            balance(c + 1)
        if c > 0:
            finish(c - 1)
    finish(chunks - 1)

    def drain(c):
        def one(row, _):
            @pl.when((row <= z) & (z < steps - 1))
            def _():
                send_copy(c, UP, row, False).wait_send()

            @pl.when((row >= z) & (z > 0))
            def _():
                send_copy(c, DOWN, row, False).wait_send()

            @pl.when(crosses(c, row))
            def _():
                send_copy(c, ACROSS, row, False).wait_send()
            return 0

        lax.fori_loop(0, steps, one, 0)

    for c in range(KEYVAL, chunks):
        drain(c)
    for c in range(chunks):
        @pl.when(twin < steps)
        def _():
            side_copy(c).wait_send()

        near_copy(c).wait_send()
        for o in range(1, outer):
            far_copy(c, o).wait_send()
    for copy in act_copies:
        copy.wait_send()

    def kv_drain(d, _):
        @pl.when(b + d < n)
        def _():
            kv_copy(d).wait_send()
        return 0

    lax.fori_loop(1, reach + 1, kv_drain, 0)


def on_device(tokens, w_query, key_value_weight, w_out, doc_lengths):
    n = lax.axis_size("blk")
    heads = lax.axis_size("heads")
    chunks = CHUNKS
    outer = heads // 2
    steps = n // LINE
    own, width = tokens.shape
    block = own * heads
    rows_in, q_cols = w_query.shape
    kv_cols = 2 * key_value_weight.shape[2]
    rows_out = w_out.shape[0]
    chunk_cols = width // chunks
    q_heads = q_cols // HEAD_SIZE
    reach = n // 4
    half = HEAD_SIZE // 2
    freqs = np.power(rope_base, -2.0 * np.arange(half) / HEAD_SIZE).astype(np.float32)
    freqs = jnp.asarray(np.concatenate([freqs, freqs])[None, :])
    bf16, f32 = jnp.bfloat16, jnp.float32
    dma = pltpu.SemaphoreType.DMA
    return pl.pallas_call(
        functools.partial(layer_kernel, n, heads, chunks),
        out_shape=jax.ShapeDtypeStruct((own, width), bf16),
        in_specs=[
            pl.BlockSpec(memory_space=pltpu.VMEM),
            pl.BlockSpec(memory_space=pl.ANY),
            pl.BlockSpec(memory_space=pltpu.VMEM),
            pl.BlockSpec(memory_space=pl.ANY),
            pl.BlockSpec(memory_space=pltpu.SMEM),
            pl.BlockSpec(memory_space=pltpu.VMEM),
        ],
        out_specs=pl.BlockSpec(memory_space=pltpu.VMEM),
        scratch_shapes=[
            pltpu.VMEM((n * rows_in, q_cols), bf16),
            pltpu.VMEM((n * rows_in, kv_cols), bf16),
            pltpu.VMEM((chunks, n, rows_out, chunk_cols), bf16),
            pltpu.VMEM((heads, own, width), bf16),
            pltpu.VMEM((block, q_cols + kv_cols), f32),
            pltpu.VMEM((block, q_cols), bf16),
            pltpu.VMEM((reach + 1, block, kv_cols), bf16),
            pltpu.VMEM((q_heads, block, 1), f32),
            pltpu.VMEM((q_heads, block, 1), f32),
            pltpu.VMEM((block, q_cols), f32),
            pltpu.VMEM((2, outer, own, q_cols), bf16),
            pltpu.VMEM((2, block, HEAD_SIZE), f32),
            pltpu.VMEM((chunks, outer, own, chunk_cols), bf16),
            pltpu.VMEM((chunks, outer, own, chunk_cols), bf16),
            pltpu.VMEM((chunks, outer, own, chunk_cols), f32),
            pltpu.VMEM((chunks, outer, own, chunk_cols), bf16),
            pltpu.VMEM((chunks, outer, own, chunk_cols), bf16),
            dma((chunks + 1,)),
            dma((2, 3, steps)),
            dma((2, n)),
            dma((chunks, 3, steps)),
            dma((chunks, n)),
            dma((chunks,)),
            dma((2 * outer,)),
            dma((heads,)),
            dma((reach + 1,)),
            dma((reach + 1,)),
            dma((chunks,)),
            dma((chunks,)),
            dma((chunks, outer)),
            dma((chunks, outer)),
        ],
        compiler_params=pltpu.CompilerParams(
            collective_id=0, has_side_effects=True, vmem_limit_bytes=60 * 1024 * 1024
        ),
    )(tokens, w_query, key_value_weight, w_out, doc_lengths, freqs)


def solution(mesh):
    return jax.shard_map(
        on_device,
        mesh=mesh,
        in_specs=(
            P(("blk", "heads"), None),
            P("blk", "heads"),
            P("blk", None, "heads"),
            P(("heads", "blk"), None),
            P(),
        ),
        out_specs=P(("blk", "heads"), None),
        check_vma=False,
    )
```

```python
import functools

import jax
import jax.numpy as jnp
import numpy as np
from jax import lax
from jax.experimental import pallas as pl
from jax.experimental.pallas import tpu as pltpu
from jax.sharding import PartitionSpec as P

HEAD_SIZE = 128
CHUNKS = 4
LINE = 2

norm_epsilon = 1e-05
rope_base = 500000.0
masked_score = -1e30
MESH = pl.DeviceIdType.MESH
UP, DOWN, ACROSS = 0, 1, 2
QUERY, KEYVAL = -1, -2


def layer_kernel(
    n, heads, chunks,
    tok_ref, w_query_ref, w_keyval_ref, w_out_ref, len_ref, freq_ref, out_ref,
    w_in, w_kv, w_proj, acts, qkv, query, kv, high, total, accum, mixed, rope,
    near_send, near_recv, part, far_send, far_recv,
    local_sem, in_send, in_recv, proj_send, proj_recv, bal_send,
    act_send, act_recv, kv_send, kv_recv, near_ss, near_rs, far_ss, far_rs,
):
    f32, bf16 = jnp.float32, jnp.bfloat16
    b = lax.axis_index("blk")
    h = lax.axis_index("heads")
    steps = n // LINE
    z, x = b // LINE, b % LINE
    outer = heads // 2
    y, core = h // 2, h % 2
    mate = y * 2 + 1 - core
    reach = n // 4
    tokens_own, width = tok_ref.shape
    rows_in = w_query_ref.shape[0]
    rows_out = w_out_ref.shape[0]
    chunk_cols = w_out_ref.shape[1] // chunks
    block = tokens_own * heads
    q_cols = query.shape[1]
    q_heads = q_cols // HEAD_SIZE

    def at_blk(i):
        return {"blk": i}

    def at_head(i):
        return {"heads": i}

    def remote(src, dst, ss, rs, dev):
        return pltpu.make_async_remote_copy(
            src_ref=src, dst_ref=dst, send_sem=ss, recv_sem=rs, device_id=dev, device_id_type=MESH
        )

    barrier = pltpu.get_barrier_semaphore()
    span = max(reach, LINE)
    peers = 0
    for d in sorted({e % n for k in range(1, span + 1) for e in (k, -k)}):
        pl.semaphore_signal(barrier, inc=1, device_id=at_blk(lax.rem(b + d, n)), device_id_type=MESH)
        peers += 1
    for d in range(1, heads):
        pl.semaphore_signal(barrier, inc=1, device_id=at_head(lax.rem(h + d, heads)), device_id_type=MESH)
        peers += 1
    pl.semaphore_wait(barrier, peers)

    def in_slot(i):
        return w_in.at[pl.ds(pl.multiple_of(i * rows_in, rows_in), rows_in)]

    def kv_slot(i):
        return w_kv.at[pl.ds(pl.multiple_of(i * rows_in, rows_in), rows_in)]

    def proj_slot(c, i):
        return w_proj.at[c, i]

    def proj_own(c):
        return w_out_ref.at[:, pl.ds(c * chunk_cols, chunk_cols)]

    def stream(c):
        if c < 0:
            slot, source = (in_slot, w_query_ref) if c == QUERY else (kv_slot, kv_slot(b))
            return slot, source, lambda d, r: in_send.at[c + 2, d, r], lambda i: in_recv.at[c + 2, i]
        return (
            functools.partial(proj_slot, c), proj_own(c),
            lambda d, r: proj_send.at[c, d, r], lambda i: proj_recv.at[c, i],
        )

    def target(direction):
        if direction == UP:
            return at_blk(lax.rem(b + LINE, n))
        if direction == DOWN:
            return at_blk(lax.rem(b + n - LINE, n))
        return at_blk(z * LINE + 1 - x)

    def send_copy(c, direction, row, own):
        slot, source, ss, rs = stream(c)
        origin = row * LINE + x
        dst = slot(origin)
        return remote(source if own else dst, dst, ss(direction, row), rs(origin), target(direction))

    def await_slot(c, origin):
        slot, source, ss, rs = stream(c)
        ref = slot(origin)
        remote(ref, ref, ss(0, 0), rs(origin), target(ACROSS)).wait_recv()

    twin = z + 1 - 2 * (z % 2)

    def crosses(c, row):
        if c < 0:
            return row >= 0
        return row != twin

    def line_own(c):
        @pl.when(z < steps - 1)
        def _():
            send_copy(c, UP, z, True).start()

        @pl.when(z > 0)
        def _():
            send_copy(c, DOWN, z, True).start()

    def line_step(c, s):
        @pl.when(z - s >= 0)
        def _():
            await_slot(c, (z - s) * LINE + x)

            @pl.when(z < steps - 1)
            def _():
                send_copy(c, UP, z - s, False).start()

        @pl.when(z + s <= steps - 1)
        def _():
            await_slot(c, (z + s) * LINE + x)

            @pl.when(z > 0)
            def _():
                send_copy(c, DOWN, z + s, False).start()

    def cross_own(c):
        send_copy(c, ACROSS, z, True).start()

    def cross_step(c, s):
        @pl.when((z - s >= 0) & crosses(c, z - s))
        def _():
            send_copy(c, ACROSS, z - s, False).start()

        @pl.when((z + s <= steps - 1) & crosses(c, z + s))
        def _():
            send_copy(c, ACROSS, z + s, False).start()

    def side_copy(c):
        ref = proj_slot(c, z * LINE + 1 - x)
        return remote(ref, ref, bal_send.at[c], proj_recv.at[c, z * LINE + 1 - x],
                      at_blk(twin * LINE + x))

    def balance(c):
        @pl.when(twin < steps)
        def _():
            await_slot(c, z * LINE + 1 - x)
            side_copy(c).start()

    def await_crossed(c):
        def one(row, _):
            if c < 0:
                await_slot(c, row * LINE + 1 - x)
            else:
                @pl.when((row != z) | (twin >= steps))
                def _():
                    await_slot(c, row * LINE + 1 - x)
            return 0

        lax.fori_loop(0, steps, one, 0)

    line_own(QUERY)
    cross_own(QUERY)
    keep_in = pltpu.make_async_copy(w_query_ref, in_slot(b), local_sem.at[chunks])
    keep_in.start()
    w_kv[pl.ds(pl.multiple_of(b * rows_in, rows_in), rows_in), :] = w_keyval_ref[...].reshape(
        rows_in, w_kv.shape[1]
    )
    line_own(KEYVAL)
    cross_own(KEYVAL)
    keep_out = [
        pltpu.make_async_copy(proj_own(c), proj_slot(c, b), local_sem.at[c]) for c in range(chunks)
    ]
    for copy in keep_out:
        copy.start()

    values = tok_ref[...].astype(f32)
    acts[h] = (
        values * lax.rsqrt(jnp.mean(values * values, axis=1, keepdims=True) + norm_epsilon)
    ).astype(bf16)

    act_copies = []
    for o in range(1, outer):
        act_copies.append(remote(acts.at[h], acts.at[h], act_send.at[o], act_recv.at[h],
                                 at_head(lax.rem(y + o, outer) * 2 + core)))
    act_copies.append(remote(acts.at[h], acts.at[h], act_send.at[0], act_recv.at[h], at_head(mate)))
    for copy in act_copies:
        copy.start()

    pos = b * block + lax.broadcasted_iota(jnp.int32, (block, 1), 0)
    start = jnp.zeros((block, 1), jnp.int32)
    end = jnp.int32(0)
    for i in range(len_ref.shape[0]):
        size = len_ref[i]
        end = end + size
        start = start + jnp.where(pos >= end, size, 0)
    angle = (pos - start).astype(f32) * freq_ref[...]
    lane = lax.broadcasted_iota(jnp.int32, (block, HEAD_SIZE), 1)
    rope[0] = jnp.cos(angle)
    rope[1] = jnp.where(lane < HEAD_SIZE // 2, -jnp.sin(angle), jnp.sin(angle))

    def in_step(s, _):
        for c in (QUERY, KEYVAL):
            line_step(c, s)
            cross_step(c, s)
        return 0

    in_step(1, 0)
    for o in range(1, outer):
        other = lax.rem(y + o, outer) * 2 + core
        remote(acts.at[other], acts.at[other], act_send.at[0], act_recv.at[other], at_head(mate)).wait_recv()
        copy = remote(acts.at[other], acts.at[other], act_send.at[outer + o], act_recv.at[other], at_head(mate))
        copy.start()
        act_copies.append(copy)
    lax.fori_loop(2, steps - 1, in_step, 0)

    for c in range(chunks):
        line_own(c)
    in_step(steps - 1, 0)
    for c in range(chunks // 2):
        cross_own(c)
    line_events = [(c, s) for s in range(1, steps) for c in range(chunks)]

    def run_events(count):
        for _ in range(min(count, len(line_events))):
            c, s = line_events.pop(0)
            line_step(c, s)

    keep_in.wait()
    for o in range(outer):
        other = lax.rem(y + o, outer) * 2 + 1 - core
        remote(acts.at[other], acts.at[other], act_send.at[0], act_recv.at[other], at_head(mate)).wait_recv()

    def project(k, size):
        cols = pl.ds(pl.multiple_of(k * size, size), size)
        left = acts[:, :, cols].reshape(block, size)
        qkv[:, :q_cols] += jnp.dot(left, w_in[cols, :], preferred_element_type=f32)
        qkv[:, q_cols:] += jnp.dot(left, w_kv[cols, :], preferred_element_type=f32)

    qkv[...] = jnp.zeros_like(qkv)

    if rows_in % HEAD_SIZE == 0:
        def lined(row, _):
            project(row * LINE + x, rows_in)
            return 0

        def crossed_row(row):
            origin = row * LINE + 1 - x
            await_slot(QUERY, origin)
            await_slot(KEYVAL, origin)
            project(origin, rows_in)

        def crossed(s, _):
            @pl.when(z - s >= 0)
            def _():
                crossed_row(z - s)

            @pl.when(z + s <= steps - 1)
            def _():
                crossed_row(z + s)
            return 0

        lax.fori_loop(0, steps, lined, 0)
        crossed_row(z)
        run_events(chunks)
        lax.fori_loop(1, steps - 1, crossed, 0)
        run_events(chunks // 2)
        crossed(steps - 1, 0)
    else:
        run_events(chunks + chunks // 2)
        await_crossed(QUERY)
        await_crossed(KEYVAL)
        depth = min(512, width)

        def whole_step(k, _):
            project(k, depth)
            return 0

        lax.fori_loop(0, width // depth, whole_step, 0)

    cosine, sine = rope[0], rope[1]

    def rotated(first):
        v = qkv[:, first:first + HEAD_SIZE]
        return (v * cosine + pltpu.roll(v, HEAD_SIZE // 2, 1) * sine).astype(bf16)

    kv[0, :, :HEAD_SIZE] = rotated(q_cols)
    kv[0, :, HEAD_SIZE:] = qkv[:, q_cols + HEAD_SIZE:].astype(bf16)
    for j in range(q_heads):
        query[:, j * HEAD_SIZE:(j + 1) * HEAD_SIZE] = rotated(j * HEAD_SIZE)

    def kv_copy(d):
        return remote(kv.at[0], kv.at[d], kv_send.at[d], kv_recv.at[d], at_blk(lax.rem(b + d, n)))

    def kv_start(d, _):
        @pl.when(b + d < n)
        def _():
            kv_copy(d).start()
        return 0

    lax.fori_loop(1, reach + 1, kv_start, 0)
    run_events(chunks - chunks // 2)

    scale = HEAD_SIZE ** (-0.5)
    high[...] = jnp.full_like(high, masked_score)
    total[...] = jnp.zeros_like(total)
    accum[...] = jnp.zeros_like(accum)
    own_pos = lax.broadcasted_iota(jnp.int32, (block, 1), 0)
    own_start = start - b * block
    key_lane = lax.broadcasted_iota(jnp.int32, (1, block), 1)

    def attend(d):
        key_pos = key_lane - d * block
        keep = (key_pos >= own_start) & (key_pos <= own_pos)

        def one(j, _):
            cols = pl.ds(pl.multiple_of(j * HEAD_SIZE, HEAD_SIZE), HEAD_SIZE)
            scores = lax.dot_general(
                query[:, cols], kv[d, :, :HEAD_SIZE], (((1,), (1,)), ((), ())),
                preferred_element_type=f32,
            ) * scale
            scores = jnp.where(keep, scores, masked_score)
            old = high[j]
            new = jnp.maximum(old, jnp.max(scores, axis=1, keepdims=True))
            fading = jnp.exp(old - new)
            probs = jnp.where(keep, jnp.exp(scores - new), 0.0)
            total[j] = total[j] * fading + jnp.sum(probs, axis=1, keepdims=True)
            update = jnp.dot(probs.astype(bf16), kv[d, :, HEAD_SIZE:], preferred_element_type=f32)
            accum[:, cols] = accum[:, cols] * fading + update
            high[j] = new
            return 0

        lax.fori_loop(0, q_heads, one, 0)

    for c in range(chunks):
        if c >= chunks // 2:
            cross_own(c)
        for s in range(1, steps):
            if (c, s) in line_events:
                line_step(c, s)
            cross_step(c, s)
        if c == 0:
            attend(0)
    early = min(2, chunks)
    for c in range(early):
        balance(c)

    def earlier(d, _):
        @pl.when(b >= d)
        def _():
            remote(kv.at[d], kv.at[d], kv_send.at[d], kv_recv.at[d], at_blk(lax.rem(b + 1, n))).wait_recv()
            attend(d)
        return 0

    lax.fori_loop(1, reach + 1, earlier, 0)

    for g in range(heads):
        rows = slice(g * tokens_own, (g + 1) * tokens_own)
        for j in range(q_heads):
            cols = slice(j * HEAD_SIZE, (j + 1) * HEAD_SIZE)
            mixed[g % 2, g // 2, :, cols] = (accum[rows, cols] / total[j, rows]).astype(bf16)

    tile = min(512, chunk_cols)

    def weight_tile(c, cols):
        right = w_proj[c, :, :, cols]
        if rows_out % 16:
            return right.astype(f32).reshape(n * rows_out, tile).astype(bf16)
        return right.reshape(n * rows_out, tile)

    def near_copy(c):
        return remote(near_send.at[c], near_recv.at[c], near_ss.at[c], near_rs.at[c], at_head(mate))

    def far_copy(c, o):
        other = lax.rem(y + o, outer)
        return remote(far_send.at[c, o], far_recv.at[c, o], far_ss.at[c, o], far_rs.at[c, o],
                      at_head(other * 2 + core))

    def project_out(c):
        keep_out[c].wait()
        await_crossed(c)

        def theirs(k, _):
            cols = pl.ds(pl.multiple_of(k * tile, tile), tile)
            left = mixed[1 - core].reshape(outer * tokens_own, q_cols)
            term = jnp.dot(left, weight_tile(c, cols), preferred_element_type=f32)
            near_send[c, :, :, cols] = term.astype(bf16).reshape(outer, tokens_own, tile)
            return 0

        def ours(k, _):
            cols = pl.ds(pl.multiple_of(k * tile, tile), tile)
            left = mixed[core].reshape(outer * tokens_own, q_cols)
            term = jnp.dot(left, weight_tile(c, cols), preferred_element_type=f32)
            part[c, :, :, cols] = term.reshape(outer, tokens_own, tile)
            return 0

        lax.fori_loop(0, chunk_cols // tile, theirs, 0)
        near_copy(c).start()
        lax.fori_loop(0, chunk_cols // tile, ours, 0)
        near_copy(c).wait_recv()
        for o in range(1, outer):
            other = lax.rem(y + o, outer)
            far_send[c, o] = (part[c, other] + near_recv[c, other].astype(f32)).astype(bf16)
            far_copy(c, o).start()

    def finish(c):
        result = part[c, y] + near_recv[c, y].astype(f32)
        for o in range(1, outer):
            far_copy(c, o).wait_recv()
            result = result + far_recv[c, o].astype(f32)
        out_ref[:, c * chunk_cols:(c + 1) * chunk_cols] = result.astype(bf16)

    for c in range(chunks):
        project_out(c)
        if early <= c + 1 < chunks:
            balance(c + 1)
        if c > 0:
            finish(c - 1)
    finish(chunks - 1)

    def drain(c):
        def one(row, _):
            @pl.when((row <= z) & (z < steps - 1))
            def _():
                send_copy(c, UP, row, False).wait_send()

            @pl.when((row >= z) & (z > 0))
            def _():
                send_copy(c, DOWN, row, False).wait_send()

            @pl.when(crosses(c, row))
            def _():
                send_copy(c, ACROSS, row, False).wait_send()
            return 0

        lax.fori_loop(0, steps, one, 0)

    for c in range(KEYVAL, chunks):
        drain(c)
    for c in range(chunks):
        @pl.when(twin < steps)
        def _():
            side_copy(c).wait_send()

        near_copy(c).wait_send()
        for o in range(1, outer):
            far_copy(c, o).wait_send()
    for copy in act_copies:
        copy.wait_send()

    def kv_drain(d, _):
        @pl.when(b + d < n)
        def _():
            kv_copy(d).wait_send()
        return 0

    lax.fori_loop(1, reach + 1, kv_drain, 0)


def on_device(tokens, w_query, key_value_weight, w_out, doc_lengths):
    n = lax.axis_size("blk")
    heads = lax.axis_size("heads")
    chunks = CHUNKS
    outer = heads // 2
    steps = n // LINE
    own, width = tokens.shape
    block = own * heads
    rows_in, q_cols = w_query.shape
    kv_cols = 2 * key_value_weight.shape[2]
    rows_out = w_out.shape[0]
    chunk_cols = width // chunks
    q_heads = q_cols // HEAD_SIZE
    reach = n // 4
    half = HEAD_SIZE // 2
    freqs = np.power(rope_base, -2.0 * np.arange(half) / HEAD_SIZE).astype(np.float32)
    freqs = jnp.asarray(np.concatenate([freqs, freqs])[None, :])
    bf16, f32 = jnp.bfloat16, jnp.float32
    dma = pltpu.SemaphoreType.DMA
    return pl.pallas_call(
        functools.partial(layer_kernel, n, heads, chunks),
        out_shape=jax.ShapeDtypeStruct((own, width), bf16),
        in_specs=[
            pl.BlockSpec(memory_space=pltpu.VMEM),
            pl.BlockSpec(memory_space=pl.ANY),
            pl.BlockSpec(memory_space=pltpu.VMEM),
            pl.BlockSpec(memory_space=pl.ANY),
            pl.BlockSpec(memory_space=pltpu.SMEM),
            pl.BlockSpec(memory_space=pltpu.VMEM),
        ],
        out_specs=pl.BlockSpec(memory_space=pltpu.VMEM),
        scratch_shapes=[
            pltpu.VMEM((n * rows_in, q_cols), bf16),
            pltpu.VMEM((n * rows_in, kv_cols), bf16),
            pltpu.VMEM((chunks, n, rows_out, chunk_cols), bf16),
            pltpu.VMEM((heads, own, width), bf16),
            pltpu.VMEM((block, q_cols + kv_cols), f32),
            pltpu.VMEM((block, q_cols), bf16),
            pltpu.VMEM((reach + 1, block, kv_cols), bf16),
            pltpu.VMEM((q_heads, block, 1), f32),
            pltpu.VMEM((q_heads, block, 1), f32),
            pltpu.VMEM((block, q_cols), f32),
            pltpu.VMEM((2, outer, own, q_cols), bf16),
            pltpu.VMEM((2, block, HEAD_SIZE), f32),
            pltpu.VMEM((chunks, outer, own, chunk_cols), bf16),
            pltpu.VMEM((chunks, outer, own, chunk_cols), bf16),
            pltpu.VMEM((chunks, outer, own, chunk_cols), f32),
            pltpu.VMEM((chunks, outer, own, chunk_cols), bf16),
            pltpu.VMEM((chunks, outer, own, chunk_cols), bf16),
            dma((chunks + 1,)),
            dma((2, 3, steps)),
            dma((2, n)),
            dma((chunks, 3, steps)),
            dma((chunks, n)),
            dma((chunks,)),
            dma((2 * outer,)),
            dma((heads,)),
            dma((reach + 1,)),
            dma((reach + 1,)),
            dma((chunks,)),
            dma((chunks,)),
            dma((chunks, outer)),
            dma((chunks, outer)),
        ],
        compiler_params=pltpu.CompilerParams(
            collective_id=0, has_side_effects=True, vmem_limit_bytes=60 * 1024 * 1024
        ),
    )(tokens, w_query, key_value_weight, w_out, doc_lengths, freqs)


def solution(mesh):
    return jax.shard_map(
        on_device,
        mesh=mesh,
        in_specs=(
            P(("blk", "heads"), None),
            P("blk", "heads"),
            P("blk", None, "heads"),
            P(("heads", "blk"), None),
            P(),
        ),
        out_specs=P(("blk", "heads"), None),
        check_vma=False,
    )
```
